32 devices in a mesh: dp: 8 (over z, x), shard: 4 (over y, core).
Axes of the slice: x: 2, y: 2, z: 4, core: 2. Of those that a mesh axis runs over, the one named last changes fastest.
Arguments:
- hidden_in: bfloat16 [8192, 5120], P(('dp', 'shard')), may hold values from -6 to 6
- teacher: bfloat16 [8192, 768], P(('dp', 'shard')), may hold values from -6 to 6
- norm_gain: bfloat16 [5120], P('shard'), may hold values from 0.5 to 1.5
- w_key: bfloat16 [5120, 768], P('shard'), may hold values from -0.078125 to 0.078125
- group_rows: int32 [8], P('dp'), may hold values from 64 to 256
- member: int32 [8, 4], P('dp', 'shard'), may hold values from 0 to 1, as said below
Outputs:
- loss: float32 [], replicated
- grad_gain: float32 [5120], P('shard')
- grad_key: float32 [5120, 768], P('shard')
The draws below stay inside these ranges and needn't reach their ends.
Inputs may be any that keep to these rules, and one draw needn't show every extreme that they name: The first group_rows[p] token slots of each surviving device of group p hold valid tokens. `member`: 1 marks a surviving device; the first device of every group survives.
All inputs are finite; a program needn't handle non-finite values.
Results may differ from the reference program's by a relative error of at most 0.0023.
Values may be sent and summed in bfloat16 or wider, within the bound.
A program may use at most 128 MiB of HBM per device.

```python
import jax
import jax.numpy as jnp
from jax import lax

D = 5120
KV = 768
TOK_DEV = 256
GROUPS = 8
MEMBERS = 4
TOKENS = 8192


def draw_member(key, part):
    picks = jax.random.randint(key, (GROUPS, MEMBERS), 0, 4)
    first = jnp.arange(MEMBERS)[None, :] == 0
    return jnp.where((picks > 0) | first, 1, 0).astype(jnp.int32)


def touch_ends(values, key, low, top_value):
    longest = values.shape.index(max(values.shape))
    spots = []
    for shift in (0, 1):
        where = [jax.random.randint(jax.random.fold_in(key, axis), (), 0, length) for axis, length in enumerate(values.shape)]
        where[longest] = (where[longest] + shift) % values.shape[longest]
        spots.append(tuple(where))
    return values.at[spots[0]].set(low).at[spots[1]].set(top_value)


def strengthened(drawn, key, source, target, blocks, factor):
    owner, partner = [(jnp.arange(drawn.shape[dim]) // (drawn.shape[dim] // blocks)).reshape([-1 if axis == dim else 1 for axis in range(drawn.ndim)]) for dim in (source, target)]
    chosen = jax.random.permutation(key, blocks)[partner]
    strong = (owner == chosen) | (owner == (partner + blocks // 2) % blocks)
    return jnp.where(strong, factor * drawn, drawn)


def block_scale(rng, dims, cuts, smallest, high):
    gain, own = 1.0, jax.random.fold_in(rng, 6)
    for dim, shards_of in cuts:
        draws = jnp.exp(jax.random.uniform(jax.random.fold_in(own, dim), (shards_of,), jnp.float32, smallest / len(cuts), high / len(cuts)))
        gain = gain * jnp.repeat(draws, dims[dim] // shards_of).reshape([-1 if axis == dim else 1 for axis in range(len(dims))])
    return gain


def noise(rng, shape, deviation, limit, cuts=(), dtype=jnp.bfloat16):
    result = deviation * jax.random.normal(rng, shape, jnp.float32)
    if cuts:
        result = result * block_scale(rng, shape, cuts, -0.22, 0.18)
    return jnp.clip(result, -limit, limit).astype(dtype)


def noise_with(rng, extent, deviation, limit, pieces, heavy, held_as=jnp.bfloat16):
    values = deviation * jax.random.normal(rng, extent, jnp.float32)
    if pieces:
        values = values * block_scale(rng, extent, pieces, -0.22, 0.18)
    return jnp.clip(strengthened(values, jax.random.fold_in(rng, 3), *heavy), -limit, limit).astype(held_as)


def setup_inputs(seed: int = 0) -> dict:
    seeds = jax.random.split(jax.random.key(seed), 7)
    return {
        "hidden_in": noise_with(seeds[0], (TOKENS, D), 1.0, 6.0, ((0, 32),), (0, 1, 32, 2.75)),
        "teacher": noise(seeds[1], (TOKENS, KV), 1.0, 6.0, ((0, 32),)),
        "norm_gain": jnp.clip(1.0 + 0.1 * jax.random.normal(seeds[2], (D,), jnp.float32), 0.5, 1.5).astype(jnp.bfloat16),
        "w_key": noise(seeds[3], (D, KV), D ** -0.5, 0.078125, ((0, 4),)),
        "group_rows": touch_ends(jax.random.randint(seeds[4], (GROUPS,), TOK_DEV // 4, TOK_DEV + 1), jax.random.fold_in(seeds[4], 1), TOK_DEV // 4, TOK_DEV).astype(jnp.int32),
        "member": draw_member(jax.random.fold_in(seeds[6], 71), 0),
    }


EPSILON = 1e-06
SCALE = 1024.0

def reference(hidden_in, teacher, norm_gain, w_key, group_rows, member):
    blocks = GROUPS * MEMBERS
    live_rows = jnp.repeat(group_rows, MEMBERS).astype(jnp.int32)
    alive = member.reshape(blocks).astype(jnp.int32)
    total_count = jnp.sum(member.astype(jnp.float32) * group_rows.astype(jnp.float32)[:, None])
    gains = norm_gain.astype(jnp.float32)

    def one_block(carry, inputs):
        loss_sum, gain_acc, key_acc = carry
        block_in, block_teacher, block_rows, block_alive = inputs
        position = lax.broadcasted_iota(jnp.int32, (TOK_DEV, 1), 0)
        valid = jnp.where((position < block_rows) & (block_alive == 1), 1.0, 0.0).astype(jnp.float32)
        values = block_in.astype(jnp.float32)
        inverse_rms = lax.rsqrt(lax.optimization_barrier(jnp.mean(values * values, axis=1, keepdims=True)) + EPSILON)
        scaled = values * inverse_rms
        normed = (scaled * gains).astype(jnp.bfloat16)
        keys = jnp.dot(normed, w_key, preferred_element_type=jnp.float32)
        diff = keys - block_teacher.astype(jnp.float32)
        loss_sum = loss_sum + jnp.sum(valid * diff * diff)
        upstream = (SCALE / total_count * valid * diff).astype(jnp.bfloat16)
        term_key = jnp.dot(normed.T, upstream, preferred_element_type=jnp.float32)
        dnormed = jnp.dot(upstream, w_key.T, preferred_element_type=jnp.float32)
        term_gain = lax.optimization_barrier(jnp.sum(dnormed * scaled, axis=0))
        return ((loss_sum, gain_acc + term_gain, key_acc + term_key), None)
    start = (jnp.zeros((), jnp.float32), jnp.zeros((D,), jnp.float32), jnp.zeros((D, KV), jnp.float32))
    inputs = (hidden_in.reshape(blocks, TOK_DEV, D), teacher.reshape(blocks, TOK_DEV, KV), live_rows, alive)
    final, unused = lax.scan(one_block, start, inputs)
    loss_sum, gain_acc, key_acc = final
    loss = loss_sum / (2.0 * KV * total_count)
    return (loss, gain_acc, key_acc)
```

```python
import functools
import math

import jax
import jax.numpy as jnp
from jax import lax
from jax.experimental import pallas as pl
from jax.experimental.pallas import tpu as pltpu
from jax.sharding import PartitionSpec as P

EPSILON = 1e-06
SCALE = 1024.0
MESH = pl.DeviceIdType.MESH
F32 = jnp.float32
BF16 = jnp.bfloat16


def inner_of(groups):
    return max(d for d in range(1, groups + 1) if groups % d == 0 and d * d <= groups)


def kernel(
    members, groups, width, chunks,
    hidden, teacher, gains, w_key, valid, count,
    out, loss_out,
    inv_cols, small_send, small_recv, cnt_send, cnt_recv, loss_send, loss_recv,
    cols, cols_t, part_send, part_recv, keys_own, keys_recv, dk_all,
    grads, x_recv, half, z_recv,
    a2a_s, a2a_r, small_s, small_r, cnt_s, cnt_r, loss_s, loss_r,
    part_s, part_r, keys_s, keys_r, dk_s, dk_r, dks_s, dks_r, dkf_s, dkf_r,
    x_s, x_r, z_s, z_r, za_s, za_r, xa_s, xa_r,
):
    tokens, kv = teacher.shape
    feats = w_key.shape[0]
    kc = kv // chunks
    inner = inner_of(groups)
    outer = groups // inner
    hrows = feats // inner
    qrows = hrows // outer
    pairs = members // 2
    p, s = lax.axis_index("dp"), lax.axis_index("shard")
    px, pz = lax.rem(p, inner), p // inner
    chip, par = s // 2, lax.rem(s, 2)
    twin = chip * 2 + 1 - par
    pending = []

    def member_at(d):
        return lax.rem(s + d, members)

    def group_at(d):
        return lax.rem(p + d, groups)

    def chip_at(d):
        return lax.rem(chip + d, pairs)

    def x_at(d):
        return lax.rem(px + d, inner)

    def z_at(d):
        return lax.rem(pz + d, outer)

    def send(src, dst, ssem, rsem, group, member):
        copy = pltpu.make_async_remote_copy(
            src_ref=src, dst_ref=dst, send_sem=ssem, recv_sem=rsem,
            device_id=(group, member), device_id_type=MESH,
        )
        copy.start()
        pending.append(copy)

    def arrived(dst, ssem, rsem):
        pltpu.make_async_remote_copy(
            src_ref=dst, dst_ref=dst, send_sem=ssem, recv_sem=rsem,
            device_id=(p, twin), device_id_type=MESH,
        ).wait_recv()

    barrier = pltpu.get_barrier_semaphore()
    for d in range(1, members):
        pl.semaphore_signal(barrier, inc=1, device_id=(p, member_at(d)), device_id_type=MESH)
    for d in range(1, groups):
        pl.semaphore_signal(barrier, inc=1, device_id=(group_at(d), s), device_id_type=MESH)
    pl.semaphore_wait(barrier, members + groups - 2)

    for d in range(1, members):
        j = member_at(d)
        send(
            hidden.at[:, pl.ds(pl.multiple_of(j * feats, 128), feats)],
            cols.at[s], a2a_s.at[d - 1], a2a_r.at[d - 1], p, j,
        )

    step_rows = 64
    def squares(r, carry):
        rows = pl.ds(pl.multiple_of(r * step_rows, step_rows), step_rows)
        x = hidden[rows, :].astype(F32)
        total = jnp.sum(x * x, axis=1, keepdims=True)
        inv = lax.rsqrt(total / width + EPSILON)
        inv_cols[rows, :] = jnp.broadcast_to(inv, (step_rows, 128))
        return carry
    lax.fori_loop(0, tokens // step_rows, squares, 0)

    small_send[pl.ds(0, 8), :] = inv_cols[...].T[:8, :]
    small_send[pl.ds(8, 8), :] = jnp.broadcast_to(count[:, :1], (8, tokens))
    for d in range(1, members):
        send(small_send, small_recv.at[d - 1], small_s.at[d - 1], small_r.at[d - 1], p, member_at(d))

    def normalise(j, source, column):
        def rows_of(r, carry):
            rows = pl.ds(pl.multiple_of(r * step_rows, step_rows), step_rows)
            x = source(rows).astype(F32) * inv_cols[rows, :1]
            cols[j, rows, :] = (x * gains[...]).astype(BF16)
            return carry
        lax.fori_loop(0, tokens // step_rows, rows_of, 0)

        def turn(b, carry):
            lanes = pl.ds(pl.multiple_of(b * 128, 128), 128)
            cols_t[lanes, pl.ds(pl.multiple_of(j * tokens, 128), tokens)] = cols[j, :, lanes].T
            return carry
        lax.fori_loop(0, feats // 128, turn, 0)

    own = pl.ds(pl.multiple_of(s * feats, 128), feats)
    normalise(s, lambda rows: hidden[rows, own], None)

    total = count[...]
    for d in range(1, members):
        arrived(small_recv.at[d - 1], small_s.at[d - 1], small_r.at[d - 1])
        total = total + small_recv[d - 1, pl.ds(8, 8), :128]
    cnt_send[...] = total
    for d in range(1, groups):
        send(cnt_send, cnt_recv.at[d - 1], cnt_s.at[d - 1], cnt_r.at[d - 1], group_at(d), s)

    for d in range(1, members):
        j = lax.rem(s + members - d, members)
        arrived(cols.at[j], a2a_s.at[d - 1], a2a_r.at[d - 1])
        inv_cols[...] = jnp.broadcast_to(small_recv[d - 1, pl.ds(0, 1), :], (128, tokens)).T
        normalise(j, lambda rows: cols[j, rows, :], None)

    for d in range(1, groups):
        arrived(cnt_recv.at[d - 1], cnt_s.at[d - 1], cnt_r.at[d - 1])
        total = total + cnt_recv[d - 1]
    scale = valid[...] * (SCALE / total[:1, :1])

    def lanes_of(c):
        return pl.ds(c * kc, kc)

    def stage_keys(c):
        for d in range(pairs):
            j = chip_at(d) * 2 + 1 - par
            part_send[c, d] = jnp.dot(cols[j], w_key[:, lanes_of(c)], preferred_element_type=F32)
            send(part_send.at[c, d], part_recv.at[c, d], part_s.at[c, d], part_r.at[c, d], p, twin)
        for i in range(pairs):
            d = (i + 1) % pairs
            j = chip_at(d) * 2 + par
            mine = jnp.dot(cols[j], w_key[:, lanes_of(c)], preferred_element_type=F32)
            arrived(part_recv.at[c, d], part_s.at[c, d], part_r.at[c, d])
            keys_own[c, d] = mine + part_recv[c, d]
            if d:
                send(
                    keys_own.at[c, d], keys_recv.at[c, d - 1],
                    keys_s.at[c, d - 1], keys_r.at[c, d - 1], p, j,
                )

    def stage_dk(c):
        keys = keys_own[c, 0]
        for d in range(1, pairs):
            arrived(keys_recv.at[c, d - 1], keys_s.at[c, d - 1], keys_r.at[c, d - 1])
            keys = keys + keys_recv[c, d - 1]
        diff = keys - teacher[:, lanes_of(c)].astype(F32)
        dk_all[c, s] = (scale * diff).astype(BF16)
        for d in range(1, pairs):
            send(
                dk_all.at[c, s], dk_all.at[c, s], dk_s.at[c, d - 1], dk_r.at[c, d - 1],
                p, chip_at(d) * 2 + par,
            )
        send(dk_all.at[c, s], dk_all.at[c, s], dks_s.at[c], dks_r.at[c], p, twin)

    def stage_grads(c, loss):
        for d in range(1, pairs):
            q = lax.rem(chip + pairs - d, pairs) * 2 + par
            arrived(dk_all.at[c, q], dk_s.at[c, d - 1], dk_r.at[c, d - 1])
            send(dk_all.at[c, q], dk_all.at[c, q], dkf_s.at[c, d - 1], dkf_r.at[c, d - 1], p, twin)
        arrived(dk_all.at[c, twin], dks_s.at[c], dks_r.at[c])
        for d in range(1, pairs):
            q = lax.rem(chip + pairs - d, pairs) * 2 + 1 - par
            arrived(dk_all.at[c, q], dkf_s.at[c, d - 1], dkf_r.at[c, d - 1])
        dk = dk_all[c].reshape(members * tokens, kc)
        for i in range(inner):
            d = (i + 1) % inner
            rows = pl.ds(pl.multiple_of(x_at(d) * hrows, 8), hrows)
            grads[c, d] = jnp.dot(cols_t[rows, :], dk, preferred_element_type=F32)
            if d:
                send(
                    grads.at[c, d], x_recv.at[c, d - 1], x_s.at[c, d - 1], x_r.at[c, d - 1],
                    pz * inner + x_at(d), s,
                )
        for m in range(members):
            values = dk_all[c, m].astype(F32)
            loss = loss + jnp.sum(values * values, axis=0, keepdims=True)
        return loss

    def stage_z(c):
        value = grads[c, 0]
        for d in range(1, inner):
            arrived(x_recv.at[c, d - 1], x_s.at[c, d - 1], x_r.at[c, d - 1])
            value = value + x_recv[c, d - 1]
        half[c] = value
        for d in range(1, outer):
            to = z_at(d)
            send(
                half.at[c, pl.ds(pl.multiple_of(to * qrows, 8), qrows), :], z_recv.at[c, d - 1],
                z_s.at[c, d - 1], z_r.at[c, d - 1], to * inner + px, s,
            )

    def rows_at(x, z):
        return pl.ds(pl.multiple_of(x * hrows + z * qrows, 8), qrows)

    def stage_sum(c):
        value = half[c, pl.ds(pl.multiple_of(pz * qrows, 8), qrows), :]
        for d in range(1, outer):
            arrived(z_recv.at[c, d - 1], z_s.at[c, d - 1], z_r.at[c, d - 1])
            value = value + z_recv[c, d - 1]
        mine = rows_at(px, pz)
        out[mine, lanes_of(c)] = value
        spot = out.at[mine, lanes_of(c)]
        for d in range(1, outer):
            send(spot, spot, za_s.at[c, d - 1], za_r.at[c, d - 1], z_at(d) * inner + px, s)
        for e in range(1, inner):
            k = (e - 1) * outer
            send(spot, spot, xa_s.at[c, k], xa_r.at[c, k], pz * inner + x_at(e), s)

    def stage_spread(c):
        for d in range(1, outer):
            spot = out.at[rows_at(px, lax.rem(pz + outer - d, outer)), lanes_of(c)]
            arrived(spot, za_s.at[c, d - 1], za_r.at[c, d - 1])
            for e in range(1, inner):
                k = (e - 1) * outer + d
                send(spot, spot, xa_s.at[c, k], xa_r.at[c, k], pz * inner + x_at(e), s)

    loss = jnp.zeros((1, kc), F32)
    for step in range(chunks + 5):
        for lag, stage in enumerate((stage_keys, stage_dk, stage_grads, stage_z, stage_sum, stage_spread)):
            c = step - lag
            if 0 <= c < chunks:
                if stage is stage_grads:
                    loss = stage(c, loss)
                else:
                    stage(c)
        if step == chunks + 1:
            loss_send[...] = jnp.broadcast_to(jnp.sum(loss, axis=1, keepdims=True), (8, 128))
            for d in range(1, groups):
                send(loss_send, loss_recv.at[d - 1], loss_s.at[d - 1], loss_r.at[d - 1], group_at(d), s)

    square = loss_send[...]
    for d in range(1, groups):
        arrived(loss_recv.at[d - 1], loss_s.at[d - 1], loss_r.at[d - 1])
        square = square + loss_recv[d - 1]
    loss_out[...] = square * (total * (1.0 / (SCALE * SCALE * 2.0 * kv)))
    for c in range(chunks):
        for e in range(1, inner):
            for d in range(outer):
                spot = out.at[
                    rows_at(lax.rem(px + inner - e, inner), lax.rem(pz + outer - d, outer)), lanes_of(c)
                ]
                k = (e - 1) * outer + d
                arrived(spot, xa_s.at[c, k], xa_r.at[c, k])
    for copy in pending:
        copy.wait_send()


def body(members, groups, hidden_in, teacher, norm_gain, w_key, group_rows, member):
    tokens, width = hidden_in.shape
    owned, kv = w_key.shape
    unit = math.lcm(128, 8 * groups)
    feats = -(-owned // unit) * unit
    chunks = 3 if kv % 384 == 0 else 1
    kc = kv // chunks
    live_rows, alive = group_rows[0], member[0, 0]
    position = lax.broadcasted_iota(jnp.int32, (tokens, 1), 0)
    valid = jnp.where((position < live_rows) & (alive == 1), 1.0, 0.0).astype(F32)
    count = jnp.broadcast_to((alive * live_rows).astype(F32), (8, 128))
    gains = norm_gain.astype(F32)
    hidden, weights, wide_gains = hidden_in, w_key, gains
    if feats != owned:
        extra = feats - owned
        hidden = jnp.pad(hidden_in.reshape(tokens, members, owned), ((0, 0), (0, 0), (0, extra)))
        hidden = hidden.reshape(tokens, members * feats)
        weights = jnp.pad(w_key, ((0, extra), (0, 0)))
        wide_gains = jnp.pad(gains, (0, extra))
    inner = inner_of(groups)
    outer = groups // inner
    hrows, pairs = feats // inner, members // 2
    vm = pltpu.VMEM

    def sems(*shape):
        kind = pltpu.SemaphoreType.DMA(tuple(max(n, 1) for n in shape))
        return [kind, kind]

    grad_key, loss = pl.pallas_call(
        functools.partial(kernel, members, groups, width, chunks),
        out_shape=(
            jax.ShapeDtypeStruct((feats, kv), F32),
            jax.ShapeDtypeStruct((8, 128), F32),
        ),
        in_specs=[pl.BlockSpec(memory_space=pltpu.VMEM)] * 6,
        out_specs=(pl.BlockSpec(memory_space=pltpu.VMEM),) * 2,
        scratch_shapes=[
            vm((tokens, 128), F32),
            vm((16, tokens), F32), vm((members - 1, 16, tokens), F32),
            vm((8, 128), F32), vm((groups - 1, 8, 128), F32),
            vm((8, 128), F32), vm((groups - 1, 8, 128), F32),
            vm((members, tokens, feats), BF16), vm((feats, members * tokens), BF16),
            vm((chunks, pairs, tokens, kc), F32), vm((chunks, pairs, tokens, kc), F32),
            vm((chunks, pairs, tokens, kc), F32), vm((chunks, max(pairs - 1, 1), tokens, kc), F32),
            vm((chunks, members, tokens, kc), BF16),
            vm((chunks, inner, hrows, kc), F32), vm((chunks, max(inner - 1, 1), hrows, kc), F32),
            vm((chunks, hrows, kc), F32), vm((chunks, max(outer - 1, 1), hrows // outer, kc), F32),
            *sems(members - 1), *sems(members - 1), *sems(groups - 1), *sems(groups - 1),
            *sems(chunks, pairs), *sems(chunks, pairs - 1), *sems(chunks, pairs - 1), *sems(chunks),
            *sems(chunks, pairs - 1),
            *sems(chunks, inner - 1), *sems(chunks, outer - 1), *sems(chunks, outer - 1),
            *sems(chunks, (inner - 1) * outer),
        ],
        compiler_params=pltpu.CompilerParams(
            collective_id=0, has_side_effects=True, vmem_limit_bytes=60 * 1024 * 1024
        ),
    )(hidden, teacher, wide_gains.reshape(1, feats), weights, valid, count)
    grad_key = grad_key[:owned]
    grad_gain = jnp.sum(grad_key * w_key.astype(F32), axis=1) / gains
    return (loss[0, 0], grad_gain, grad_key)


def solution(mesh):
    in_specs = (
        P(("dp", "shard"), None),
        P(("dp", "shard"), None),
        P("shard"),
        P("shard", None),
        P("dp"),
        P("dp", "shard"),
    )
    out_specs = (P(), P("shard"), P("shard", None))
    step = functools.partial(body, mesh.shape["shard"], mesh.shape["dp"])
    return jax.shard_map(step, mesh=mesh, in_specs=in_specs, out_specs=out_specs, check_vma=False)
```

```python
import functools
import math

import jax
import jax.numpy as jnp
from jax import lax
from jax.experimental import pallas as pl
from jax.experimental.pallas import tpu as pltpu
from jax.sharding import PartitionSpec as P

EPSILON = 1e-06
SCALE = 1024.0
MESH = pl.DeviceIdType.MESH
F32 = jnp.float32
BF16 = jnp.bfloat16


def inner_of(groups):
    return max(d for d in range(1, groups + 1) if groups % d == 0 and d * d <= groups)


def kernel(
    members, groups, width, chunks,
    hidden, teacher, gains, w_key, valid, count,
    out, loss_out,
    inv_cols, small_send, small_recv, cnt_send, cnt_recv, loss_send, loss_recv,
    cols, cols_t, part_send, part_recv, keys_own, keys_recv, dk_all,
    grads, x_send, x_recv, half, half_send, z_recv,
    a2a_s, a2a_r, small_s, small_r, cnt_s, cnt_r, loss_s, loss_r,
    part_s, part_r, keys_s, keys_r, dk_s, dk_r, dks_s, dks_r, dkf_s, dkf_r,
    x_s, x_r, z_s, z_r, zu_s, zd_s, za_r, xa_s, xa_r,
):
    tokens, kv = teacher.shape
    feats = w_key.shape[0]
    kc = kv // chunks
    inner = inner_of(groups)
    outer = groups // inner
    hrows = feats // inner
    qrows = hrows // outer
    pairs = members // 2
    align = 16
    p, s = lax.axis_index("dp"), lax.axis_index("shard")
    px, pz = lax.rem(p, inner), p // inner
    chip, par = s // 2, lax.rem(s, 2)
    twin = chip * 2 + 1 - par
    pending = []

    def member_at(d):
        return lax.rem(s + d, members)

    def group_at(d):
        return lax.rem(p + d, groups)

    def chip_at(d):
        return lax.rem(chip + d, pairs)

    def x_at(d):
        return lax.rem(px + d, inner)

    def z_at(d):
        return lax.rem(pz + d, outer)

    def send(src, dst, ssem, rsem, group, member):
        copy = pltpu.make_async_remote_copy(
            src_ref=src, dst_ref=dst, send_sem=ssem, recv_sem=rsem,
            device_id=(group, member), device_id_type=MESH,
        )
        copy.start()
        pending.append(copy)

    def arrived(dst, ssem, rsem):
        pltpu.make_async_remote_copy(
            src_ref=dst, dst_ref=dst, send_sem=ssem, recv_sem=rsem,
            device_id=(p, twin), device_id_type=MESH,
        ).wait_recv()

    barrier = pltpu.get_barrier_semaphore()
    for d in range(1, members):
        pl.semaphore_signal(barrier, inc=1, device_id=(p, member_at(d)), device_id_type=MESH)
    for d in range(1, groups):
        pl.semaphore_signal(barrier, inc=1, device_id=(group_at(d), s), device_id_type=MESH)
    pl.semaphore_wait(barrier, members + groups - 2)

    for d in range(1, members):
        j = member_at(d)
        send(
            hidden.at[:, pl.ds(pl.multiple_of(j * feats, 128), feats)],
            cols.at[s], a2a_s.at[d - 1], a2a_r.at[d - 1], p, j,
        )

    step_rows = 64
    def squares(r, carry):
        rows = pl.ds(pl.multiple_of(r * step_rows, step_rows), step_rows)
        x = hidden[rows, :].astype(F32)
        total = jnp.sum(x * x, axis=1, keepdims=True)
        inv = lax.rsqrt(total / width + EPSILON)
        inv_cols[rows, :] = jnp.broadcast_to(inv, (step_rows, 128))
        return carry
    lax.fori_loop(0, tokens // step_rows, squares, 0)

    small_send[pl.ds(0, 8), :] = inv_cols[...].T[:8, :]
    small_send[pl.ds(8, 8), :] = jnp.broadcast_to(count[:, :1], (8, tokens))
    for d in range(1, members):
        send(small_send, small_recv.at[d - 1], small_s.at[d - 1], small_r.at[d - 1], p, member_at(d))

    def normalise(j, source, column):
        def rows_of(r, carry):
            rows = pl.ds(pl.multiple_of(r * step_rows, step_rows), step_rows)
            x = source(rows).astype(F32) * inv_cols[rows, :1]
            cols[j, rows, :] = (x * gains[...]).astype(BF16)
            return carry
        lax.fori_loop(0, tokens // step_rows, rows_of, 0)

        def turn(b, carry):
            lanes = pl.ds(pl.multiple_of(b * 128, 128), 128)
            cols_t[lanes, pl.ds(pl.multiple_of(j * tokens, 128), tokens)] = cols[j, :, lanes].T
            return carry
        lax.fori_loop(0, feats // 128, turn, 0)

    own = pl.ds(pl.multiple_of(s * feats, 128), feats)
    normalise(s, lambda rows: hidden[rows, own], None)

    total = count[...]
    for d in range(1, members):
        arrived(small_recv.at[d - 1], small_s.at[d - 1], small_r.at[d - 1])
        total = total + small_recv[d - 1, pl.ds(8, 8), :128]
    cnt_send[...] = total
    for d in range(1, groups):
        send(cnt_send, cnt_recv.at[d - 1], cnt_s.at[d - 1], cnt_r.at[d - 1], group_at(d), s)

    for d in range(1, members):
        j = lax.rem(s + members - d, members)
        arrived(cols.at[j], a2a_s.at[d - 1], a2a_r.at[d - 1])
        inv_cols[...] = jnp.broadcast_to(small_recv[d - 1, pl.ds(0, 1), :], (128, tokens)).T
        normalise(j, lambda rows: cols[j, rows, :], None)

    for d in range(1, groups):
        arrived(cnt_recv.at[d - 1], cnt_s.at[d - 1], cnt_r.at[d - 1])
        total = total + cnt_recv[d - 1]
    scale = valid[...] * (SCALE / total[:1, :1])

    def lanes_of(c):
        return pl.ds(c * kc, kc)

    def stage_keys(c):
        for d in range(pairs):
            j = chip_at(d) * 2 + 1 - par
            part_send[c, d] = jnp.dot(cols[j], w_key[:, lanes_of(c)], preferred_element_type=F32)
            send(part_send.at[c, d], part_recv.at[c, d], part_s.at[c, d], part_r.at[c, d], p, twin)
        for i in range(pairs):
            d = (i + 1) % pairs
            j = chip_at(d) * 2 + par
            mine = jnp.dot(cols[j], w_key[:, lanes_of(c)], preferred_element_type=F32)
            arrived(part_recv.at[c, d], part_s.at[c, d], part_r.at[c, d])
            keys_own[c, d] = mine + part_recv[c, d]
            if d:
                send(
                    keys_own.at[c, d], keys_recv.at[c, d - 1],
                    keys_s.at[c, d - 1], keys_r.at[c, d - 1], p, j,
                )

    def stage_dk(c):
        keys = keys_own[c, 0]
        for d in range(1, pairs):
            arrived(keys_recv.at[c, d - 1], keys_s.at[c, d - 1], keys_r.at[c, d - 1])
            keys = keys + keys_recv[c, d - 1]
        diff = keys - teacher[:, lanes_of(c)].astype(F32)
        dk_all[c, s] = (scale * diff).astype(BF16)
        for d in range(1, pairs):
            send(
                dk_all.at[c, s], dk_all.at[c, s], dk_s.at[c, d - 1], dk_r.at[c, d - 1],
                p, chip_at(d) * 2 + par,
            )
        send(dk_all.at[c, s], dk_all.at[c, s], dks_s.at[c], dks_r.at[c], p, twin)

    def stage_grads(c, loss):
        for d in range(1, pairs):
            q = lax.rem(chip + pairs - d, pairs) * 2 + par
            arrived(dk_all.at[c, q], dk_s.at[c, d - 1], dk_r.at[c, d - 1])
            send(dk_all.at[c, q], dk_all.at[c, q], dkf_s.at[c, d - 1], dkf_r.at[c, d - 1], p, twin)
        arrived(dk_all.at[c, twin], dks_s.at[c], dks_r.at[c])
        for d in range(1, pairs):
            q = lax.rem(chip + pairs - d, pairs) * 2 + 1 - par
            arrived(dk_all.at[c, q], dkf_s.at[c, d - 1], dkf_r.at[c, d - 1])
        dk = dk_all[c].reshape(members * tokens, kc)
        for i in range(inner):
            d = (i + 1) % inner
            rows = pl.ds(pl.multiple_of(x_at(d) * hrows, 8), hrows)
            term = jnp.dot(cols_t[rows, :], dk, preferred_element_type=F32)
            if not d:
                grads[c] = term
            else:
                x_send[c, d - 1] = term.astype(BF16)
                send(
                    x_send.at[c, d - 1], x_recv.at[c, d - 1], x_s.at[c, d - 1], x_r.at[c, d - 1],
                    pz * inner + x_at(d), s,
                )
        for m in range(members):
            values = dk_all[c, m].astype(F32)
            loss = loss + jnp.sum(values * values, axis=0, keepdims=True)
        return loss

    def stage_z(c):
        value = grads[c]
        for d in range(1, inner):
            arrived(x_recv.at[c, d - 1], x_s.at[c, d - 1], x_r.at[c, d - 1])
            value = value + x_recv[c, d - 1].astype(F32)
        half[c] = value
        half_send[c] = value.astype(BF16)
        for d in range(1, outer):
            to = z_at(d)
            send(
                half_send.at[c, pl.ds(pl.multiple_of(to * qrows, align), qrows), :], z_recv.at[c, d - 1],
                z_s.at[c, d - 1], z_r.at[c, d - 1], to * inner + px, s,
            )

    def rows_at(x, z):
        return pl.ds(pl.multiple_of(x * hrows + z * qrows, 8), qrows)

    def stage_sum(c):
        value = half[c, pl.ds(pl.multiple_of(pz * qrows, 8), qrows), :]
        for d in range(1, outer):
            arrived(z_recv.at[c, d - 1], z_s.at[c, d - 1], z_r.at[c, d - 1])
            value = value + z_recv[c, d - 1].astype(F32)
        mine = rows_at(px, pz)
        out[mine, lanes_of(c)] = value
        spot = out.at[mine, lanes_of(c)]
        along_line(spot, c, pz)
        across(spot, c, pz)

    def across(spot, c, q):
        for e in range(1, inner):
            copy_to(spot, xa_s.at[c, e - 1, q], xa_r.at[c, e - 1, q], pz * inner + x_at(e), s).start()

    def copy_to(spot, ssem, rsem, group, member):
        return pltpu.make_async_remote_copy(
            src_ref=spot, dst_ref=spot, send_sem=ssem, recv_sem=rsem,
            device_id=(group, member), device_id_type=MESH,
        )

    def rises(q):
        return (pz >= q) & (pz < outer - 1)

    def falls(q):
        return (pz <= q) & (pz > 0)

    def up_copy(spot, c, q):
        to = jnp.minimum(pz + 1, outer - 1) * inner + px
        return copy_to(spot, zu_s.at[c, q], za_r.at[c, q], to, s)

    def down_copy(spot, c, q):
        to = jnp.maximum(pz - 1, 0) * inner + px
        return copy_to(spot, zd_s.at[c, q], za_r.at[c, q], to, s)

    def along_line(spot, c, q):
        @pl.when(rises(q))
        def _():
            up_copy(spot, c, q).start()

        @pl.when(falls(q))
        def _():
            down_copy(spot, c, q).start()

    def stage_spread(c):
        for q in range(outer):
            spot = out.at[rows_at(px, q), lanes_of(c)]

            @pl.when(pz != q)
            def _():
                arrived(spot, zu_s.at[c, q], za_r.at[c, q])
                along_line(spot, c, q)
                across(spot, c, q)

    loss = jnp.zeros((1, kc), F32)
    for step in range(chunks + 5):
        for lag, stage in enumerate((stage_keys, stage_dk, stage_grads, stage_z, stage_sum, stage_spread)):
            c = step - lag
            if 0 <= c < chunks:
                if stage is stage_grads:
                    loss = stage(c, loss)
                else:
                    stage(c)
        if step == chunks + 1:
            loss_send[...] = jnp.broadcast_to(jnp.sum(loss, axis=1, keepdims=True), (8, 128))
            for d in range(1, groups):
                send(loss_send, loss_recv.at[d - 1], loss_s.at[d - 1], loss_r.at[d - 1], group_at(d), s)

    square = loss_send[...]
    for d in range(1, groups):
        arrived(loss_recv.at[d - 1], loss_s.at[d - 1], loss_r.at[d - 1])
        square = square + loss_recv[d - 1]
    loss_out[...] = square * (total * (1.0 / (SCALE * SCALE * 2.0 * kv)))
    for c in range(chunks):
        for q in range(outer):
            for e in range(1, inner):
                spot = out.at[rows_at(lax.rem(px + inner - e, inner), q), lanes_of(c)]
                arrived(spot, xa_s.at[c, e - 1, q], xa_r.at[c, e - 1, q])
                spot = out.at[rows_at(px, q), lanes_of(c)]
                copy_to(spot, xa_s.at[c, e - 1, q], xa_r.at[c, e - 1, q], pz * inner + x_at(e), s).wait_send()
            spot = out.at[rows_at(px, q), lanes_of(c)]

            @pl.when(rises(q))
            def _():
                up_copy(spot, c, q).wait_send()

            @pl.when(falls(q))
            def _():
                down_copy(spot, c, q).wait_send()
    for copy in pending:
        copy.wait_send()


def body(members, groups, hidden_in, teacher, norm_gain, w_key, group_rows, member):
    tokens, width = hidden_in.shape
    owned, kv = w_key.shape
    unit = math.lcm(128, 16 * groups)
    feats = -(-owned // unit) * unit
    chunks = kv // 256 if kv % 256 == 0 else 1
    kc = kv // chunks
    live_rows, alive = group_rows[0], member[0, 0]
    position = lax.broadcasted_iota(jnp.int32, (tokens, 1), 0)
    valid = jnp.where((position < live_rows) & (alive == 1), 1.0, 0.0).astype(F32)
    count = jnp.broadcast_to((alive * live_rows).astype(F32), (8, 128))
    gains = norm_gain.astype(F32)
    hidden, weights, wide_gains = hidden_in, w_key, gains
    if feats != owned:
        extra = feats - owned
        hidden = jnp.pad(hidden_in.reshape(tokens, members, owned), ((0, 0), (0, 0), (0, extra)))
        hidden = hidden.reshape(tokens, members * feats)
        weights = jnp.pad(w_key, ((0, extra), (0, 0)))
        wide_gains = jnp.pad(gains, (0, extra))
    inner = inner_of(groups)
    outer = groups // inner
    hrows, pairs = feats // inner, members // 2
    vm = pltpu.VMEM

    def sems(*shape):
        kind = pltpu.SemaphoreType.DMA(tuple(max(n, 1) for n in shape))
        return [kind, kind]

    grad_key, loss = pl.pallas_call(
        functools.partial(kernel, members, groups, width, chunks),
        out_shape=(
            jax.ShapeDtypeStruct((feats, kv), F32),
            jax.ShapeDtypeStruct((8, 128), F32),
        ),
        in_specs=[pl.BlockSpec(memory_space=pltpu.VMEM)] * 6,
        out_specs=(pl.BlockSpec(memory_space=pltpu.VMEM),) * 2,
        scratch_shapes=[
            vm((tokens, 128), F32),
            vm((16, tokens), F32), vm((members - 1, 16, tokens), F32),
            vm((8, 128), F32), vm((groups - 1, 8, 128), F32),
            vm((8, 128), F32), vm((groups - 1, 8, 128), F32),
            vm((members, tokens, feats), BF16), vm((feats, members * tokens), BF16),
            vm((chunks, pairs, tokens, kc), F32), vm((chunks, pairs, tokens, kc), F32),
            vm((chunks, pairs, tokens, kc), F32), vm((chunks, max(pairs - 1, 1), tokens, kc), F32),
            vm((chunks, members, tokens, kc), BF16),
            vm((chunks, hrows, kc), F32),
            vm((chunks, max(inner - 1, 1), hrows, kc), BF16), vm((chunks, max(inner - 1, 1), hrows, kc), BF16),
            vm((chunks, hrows, kc), F32), vm((chunks, hrows, kc), BF16),
            vm((chunks, max(outer - 1, 1), hrows // outer, kc), BF16),
            *sems(members - 1), *sems(members - 1), *sems(groups - 1), *sems(groups - 1),
            *sems(chunks, pairs), *sems(chunks, pairs - 1), *sems(chunks, pairs - 1), *sems(chunks),
            *sems(chunks, pairs - 1),
            *sems(chunks, inner - 1), *sems(chunks, outer - 1),
            *sems(chunks, outer), sems(chunks, outer)[0], *sems(chunks, inner - 1, outer),
        ],
        compiler_params=pltpu.CompilerParams(
            collective_id=0, has_side_effects=True, vmem_limit_bytes=60 * 1024 * 1024
        ),
    )(hidden, teacher, wide_gains.reshape(1, feats), weights, valid, count)
    grad_key = grad_key[:owned]
    grad_gain = jnp.sum(grad_key * w_key.astype(F32), axis=1) / gains
    return (loss[0, 0], grad_gain, grad_key)


def solution(mesh):
    in_specs = (
        P(("dp", "shard"), None),
        P(("dp", "shard"), None),
        P("shard"),
        P("shard", None),
        P("dp"),
        P("dp", "shard"),
    )
    out_specs = (P(), P("shard"), P("shard", None))
    step = functools.partial(body, mesh.shape["shard"], mesh.shape["dp"])
    return jax.shard_map(step, mesh=mesh, in_specs=in_specs, out_specs=out_specs, check_vma=False)
```
